32 devices in a mesh: gx: 4 (over y, x), gy: 8 (over z, core).
Axes of the slice: x: 2, y: 2, z: 4, core: 2. Of those that a mesh axis runs over, the one named last changes fastest.
Arguments:
- sources: bfloat16 [1024, 64, 512], P(('gx', 'gy')), may hold values from -6 to 6
- projection: bfloat16 [512, 512], replicated, may hold values from -0.25 to 0.25
- translations: bfloat16 [5, 2, 512, 512], replicated, may hold values from -0.1875 to 0.1875
- angles: float32 [6, 1024, 256], P(None, ('gx', 'gy')), may hold values from -3.140625 to 3.140625
- interpolation: bfloat16 [256, 1024], replicated, may hold values from -0.25 to 0.25
- box_order: int32 [1024], P(('gx', 'gy')), may hold values from 0 to 1023, as said below
Outputs:
- targets: bfloat16 [1024, 128, 512], P(('gx', 'gy'))
The draws below stay inside these ranges and needn't reach their ends.
Inputs may be any that keep to these rules, and one draw needn't show every extreme that they name: `box_order`: each aligned block of 32 entries (entries k * 32 to (k + 1) * 32 - 1) is a permutation of those same indices.
All inputs are finite; a program needn't handle non-finite values.
Results may differ from the reference program's by a relative error of at most 0.014.
Values may be sent and summed in bfloat16 or wider, within the bound.
A program may use at most 64 MiB of HBM per device.

```python
import jax
import jax.numpy as jnp
from jax import lax

K = 256
RHS = 64
POINTS = 512
BOX_DEV = 32
LEVELS = 5
BOXES = 1024
N_GX = 4
N_GY = 8


def draw_box_order(key, part):
    blocks = BOXES // BOX_DEV
    keys = jax.random.split(jax.random.fold_in(key, 17), blocks)
    orders = jax.vmap(lambda sub_key: jax.random.permutation(sub_key, BOX_DEV))(keys)
    offsets = jnp.arange(blocks, dtype=jnp.int32)[:, None] * BOX_DEV
    return (orders.astype(jnp.int32) + offsets).reshape(-1)


def levels(key, shape, cuts, least, high):
    gain = 1.0
    for dim, parts in cuts:
        draws = jax.random.uniform(jax.random.fold_in(jax.random.fold_in(key, 6), dim), (parts,), jnp.float32, least / len(cuts), high / len(cuts))
        gain = gain * jnp.repeat(jnp.exp(draws), shape[dim] // parts).reshape((-1,) + (1,) * (len(shape) - 1 - dim))
    return gain


def noise(key, shape, scale, bound, shards=(), kind=jnp.bfloat16):
    result = jax.random.normal(key, shape, jnp.float32) * scale
    if len(shards) > 0:
        result = levels(key, shape, shards, -0.22, 0.18) * result
    return jnp.clip(result, min=-bound, max=bound).astype(kind)


def setup_inputs(seed: int = 0) -> dict:
    splits = jax.random.split(jax.random.key(seed), 7)
    return {
        "sources": noise(splits[0], (BOXES, RHS, POINTS), 1.0, 6.0, ((0, 32),)),
        "projection": noise(splits[1], (POINTS, 2 * K), POINTS ** -0.5, 0.25),
        "translations": noise(splits[2], (LEVELS, 2, 2 * K, 2 * K), (4 * K) ** -0.5, 0.1875),
        "angles": jnp.clip(jax.random.uniform(splits[3], (LEVELS + 1, BOXES, K), jnp.float32, -3.140625, 3.140625), -3.140625, 3.140625),
        "interpolation": noise(splits[4], (K, 2 * POINTS), (2 * K) ** -0.5, 0.25),
        "box_order": draw_box_order(jax.random.fold_in(splits[6], 71), 0),
    }


def mix_parts(product, coeffs, sides):
    first_part = product[..., :coeffs]
    second_part = product[..., coeffs:]
    real_part = first_part[..., :sides, :] - second_part[..., sides:, :]
    imag_part = first_part[..., sides:, :] + second_part[..., :sides, :]
    return real_part, imag_part


def rotate(real_part, imag_part, angle_row):
    cosine = jnp.cos(angle_row)[..., None, :]
    sine_part = jnp.sin(angle_row)[..., None, :]
    return jnp.concatenate([cosine * real_part - sine_part * imag_part, sine_part * real_part + cosine * imag_part], axis=-2)


def level_plan(count_x, count_y):
    bits_x = count_x.bit_length() - 1
    bits_y = count_y.bit_length() - 1
    return [("gy", bits_y - 1), ("gx", bits_x - 1), ("gy", bits_y - 2), ("gx", bits_x - 2), ("gy", bits_y - 3)]


def interpolate(coeff_state, interpolation, sides, points):
    product = jnp.einsum("bck,kq->bcq", coeff_state.astype(jnp.float32), interpolation.astype(jnp.float32))
    real_part = product[:, :sides, :points] - product[:, sides:, points:]
    imag_part = product[:, :sides, points:] + product[:, sides:, :points]
    return jnp.concatenate([real_part, imag_part], axis=1).astype(jnp.bfloat16)


def reference(sources, projection, translations, angles, interpolation, box_order):
    devices = N_GX * N_GY

    def project(packed):
        source_block, order_block, angle_block = packed
        product = jnp.einsum("brp,pk->brk", source_block.astype(jnp.float32), projection.astype(jnp.float32))
        stacked = jnp.concatenate([product[..., :K], product[..., K:]], axis=1)
        placed = jnp.zeros_like(stacked).at[(order_block % BOX_DEV).astype(jnp.int32)].set(stacked)
        return rotate(placed[:, :RHS], placed[:, RHS:], angle_block).astype(jnp.bfloat16)

    coeff_state = lax.map(project, (sources.reshape(devices, BOX_DEV, RHS, POINTS), box_order.reshape(devices, BOX_DEV), angles[0].reshape(devices, BOX_DEV, K)))
    coeff_state = coeff_state.reshape(N_GX, N_GY, BOX_DEV, 2 * RHS, K)
    for level_no, (axis_name, bit_pos) in enumerate(level_plan(N_GX, N_GY)):
        dim_no = 0 if axis_name == "gx" else 1
        stride = 1 << bit_pos
        leading = jnp.moveaxis(coeff_state, dim_no, 0)
        extent = leading.shape[0]
        grouped = leading.reshape((extent // (2 * stride), 2, stride) + leading.shape[1:])
        angle_now = jnp.moveaxis(angles[level_no + 1].reshape(N_GX, N_GY, BOX_DEV, K), dim_no, 0)
        angle_now = angle_now.reshape((extent // (2 * stride), 2, stride) + angle_now.shape[1:])
        joined = jnp.concatenate([grouped[:, 0], grouped[:, 1]], axis=-1).astype(jnp.float32)
        halves = []
        for half_bit in range(2):
            product = jnp.einsum("...k,kq->...q", joined, translations[level_no, half_bit].astype(jnp.float32))
            real_part, imag_part = mix_parts(product, K, RHS)
            halves.append(rotate(real_part, imag_part, angle_now[:, half_bit]).astype(jnp.bfloat16))
        coeff_state = jnp.moveaxis(jnp.stack(halves, axis=1).reshape(leading.shape), 0, dim_no)
    per_peer = BOX_DEV // N_GY
    regrouped = coeff_state.reshape(N_GX, N_GY, N_GY, per_peer, 2 * RHS, K).transpose(0, 2, 1, 3, 4, 5)
    regrouped = regrouped.reshape(devices, BOX_DEV, 2 * RHS, K)
    targets = lax.map(lambda device_block: interpolate(device_block, interpolation, RHS, POINTS), regrouped)
    return targets.reshape(BOXES, 2 * RHS, POINTS)
```

```python
import functools

import jax
import jax.numpy as jnp
from jax import lax
from jax.experimental import pallas as pl
from jax.experimental.pallas import tpu as pltpu
from jax.sharding import PartitionSpec as P

SPLITS = 2


def level_plan(count_x, count_y):
    bits_x = count_x.bit_length() - 1
    bits_y = count_y.bit_length() - 1
    return [
        ("gy", bits_y - 1),
        ("gx", bits_x - 1),
        ("gy", bits_y - 2),
        ("gx", bits_x - 2),
        ("gy", bits_y - 3),
    ]


def kernel(
    count_x, count_y, per_peer, sides,
    inv_ref, src_ref, proj_ref, w_ref, cos0_ref, sin0_ref, ang_ref, interp_ref,
    out_ref,
    st0, got0, st1, got1, st2, got2, tmp_a, tmp_b, ang_got, cs, sn,
    a2a_send, a2a_recv, ang_send, ang_recv, ex_send, ex_recv,
):
    f32, bf16 = jnp.float32, jnp.bfloat16
    plan = level_plan(count_x, count_y)
    levels = len(plan)
    me_x = lax.axis_index("gx")
    me_y = lax.axis_index("gy")
    half = sides // SPLITS
    rows = 2 * half
    coeffs = st0.shape[-1]
    points = interp_ref.shape[1] // 2
    chunks = per_peer * SPLITS
    x_bits = [bit for axis, bit in plan if axis == "gx"]
    x_hbs = [(me_x // (1 << bit)) % 2 for bit in x_bits]
    partners = [me_x + (1 - 2 * hb) * (1 << bit) for hb, bit in zip(x_hbs, x_bits)]

    barrier = pltpu.get_barrier_semaphore()
    for k in range(1, count_y):
        pl.semaphore_signal(
            barrier, inc=1, device_id=(me_x, (me_y + k) % count_y),
            device_id_type=pl.DeviceIdType.MESH,
        )
    for partner in partners:
        pl.semaphore_signal(
            barrier, inc=1, device_id=(partner, me_y), device_id_type=pl.DeviceIdType.MESH
        )
    pl.semaphore_wait(barrier, count_y - 1 + len(partners))

    def ang_copy(k):
        peer = (me_y + k) % count_y
        return pltpu.make_async_remote_copy(
            src_ref=ang_ref.at[peer], dst_ref=ang_got.at[me_y],
            send_sem=ang_send.at[k], recv_sem=ang_recv.at[k],
            device_id=(me_x, peer), device_id_type=pl.DeviceIdType.MESH,
        )

    def a2a_copy(c, k):
        peer = (me_y + k) % count_y
        return pltpu.make_async_remote_copy(
            src_ref=st0.at[c, peer], dst_ref=got0.at[c, me_y],
            send_sem=a2a_send.at[c, k], recv_sem=a2a_recv.at[c, k],
            device_id=(me_x, peer), device_id_type=pl.DeviceIdType.MESH,
        )

    def swap_copy(which, c):
        source, target = ((st1, got1), (st2, got2))[which]
        return pltpu.make_async_remote_copy(
            src_ref=source.at[c], dst_ref=target.at[c],
            send_sem=ex_send.at[which, c], recv_sem=ex_recv.at[which, c],
            device_id=(partners[which], me_y), device_id_type=pl.DeviceIdType.MESH,
        )

    for k in range(1, count_y):
        ang_copy(k).start()
    ang_got[me_y] = ang_ref[me_y]

    def put(store, real, imag, cosine, sine):
        store(0, (cosine * real - sine * imag).astype(bf16))
        store(half, (sine * real + cosine * imag).astype(bf16))

    def project(c):
        r, q = c // SPLITS, c % SPLITS
        first = pl.multiple_of(q * half, half)
        group = jnp.concatenate(
            [src_ref[inv_ref[p * per_peer + r], pl.ds(first, half), :] for p in range(count_y)],
            axis=0,
        )
        prod = jnp.dot(group, proj_ref[...], preferred_element_type=f32)
        for p in range(count_y):
            block = prod[p * half : (p + 1) * half]

            def store(at, value, p=p):
                st0[c, p, at : at + half, :] = value

            slot = p * per_peer + r
            put(
                store, block[:, :coeffs], block[:, coeffs:],
                cos0_ref[pl.ds(slot, 1), :], sin0_ref[pl.ds(slot, 1), :],
            )

    def finish(prod, index, y, r, level, store):
        base = index * rows
        upper = prod[base : base + half]
        lower = prod[base + half : base + rows]
        real = upper[:, :coeffs] - lower[:, coeffs:]
        imag = lower[:, :coeffs] + upper[:, coeffs:]
        row = r * levels + level
        put(store, real, imag, cs[y, pl.ds(row, 1), :], sn[y, pl.ds(row, 1), :])

    def y_level(load, make_store, level, r):
        stride = 1 << plan[level][1]
        lows = [y for y in range(count_y) if (y // stride) % 2 == 0]
        low = jnp.concatenate([load(y) for y in lows], axis=0)
        high = jnp.concatenate([load(y + stride) for y in lows], axis=0)
        for h in range(2):
            prod = jnp.dot(low, w_ref[level, h, 0], preferred_element_type=f32)
            prod += jnp.dot(high, w_ref[level, h, 1], preferred_element_type=f32)
            for index, y in enumerate(lows):
                finish(prod, index, y + h * stride, r, level, make_store(y + h * stride))

    def x_level(mine, other, which, level, r, make_store):
        hb = x_hbs[which]
        prod = jnp.dot(mine, w_ref[level, hb, hb], preferred_element_type=f32)
        prod += jnp.dot(other, w_ref[level, hb, 1 - hb], preferred_element_type=f32)
        for y in range(count_y):
            finish(prod, y, y, r, level, make_store(y))

    def into(ref):
        def make_store(y):
            def store(at, value):
                ref[y, at : at + half, :] = value

            return store

        return make_store

    def into_chunk(ref, c):
        def make_store(y):
            def store(at, value):
                ref[c, y, at : at + half, :] = value

            return store

        return make_store

    def flat(value):
        return value.reshape(count_y * rows, coeffs)

    @pl.loop(0, chunks)
    def _(c):
        project(c)
        for k in range(1, count_y):
            a2a_copy(c, k).start()
        got0[c, me_y] = st0[c, me_y]

    for k in range(1, count_y):
        ang_copy(k).wait()
    for y in range(count_y):
        angle = ang_got[y]
        cs[y] = jnp.cos(angle)
        sn[y] = jnp.sin(angle)

    @pl.loop(0, chunks + 3)
    def _(t):
        @pl.when(t < chunks)
        def _():
            c = t
            for k in range(1, count_y):
                a2a_copy(c, k).wait()
            y_level(lambda y: got0[c, y], into_chunk(st1, c), 0, c // SPLITS)
            swap_copy(0, c).start()

        @pl.when((t >= 1) & (t < chunks + 1))
        def _():
            c = t - 1
            r = c // SPLITS
            swap_copy(0, c).wait()
            x_level(flat(st1[c]), flat(got1[c]), 0, 1, r, into(tmp_a))
            y_level(lambda y: tmp_a[y], into_chunk(st2, c), 2, r)
            swap_copy(1, c).start()

        @pl.when(t >= 3)
        def _():
            c = t - 3
            r, q = c // SPLITS, c % SPLITS
            swap_copy(1, c).wait()
            x_level(flat(st2[c]), flat(got2[c]), 1, 3, r, into(tmp_a))
            y_level(lambda y: tmp_a[y], into(tmp_b), 4, r)
            prod = jnp.dot(flat(tmp_b[...]), interp_ref[...], preferred_element_type=f32)
            first = pl.multiple_of(q * half, half)
            for y in range(count_y):
                upper = prod[y * rows : y * rows + half]
                lower = prod[y * rows + half : (y + 1) * rows]
                real = upper[:, :points] - lower[:, points:]
                imag = upper[:, points:] + lower[:, :points]
                out_ref[y * per_peer + r, pl.ds(first, half), :] = real.astype(bf16)
                out_ref[y * per_peer + r, pl.ds(first + sides, half), :] = imag.astype(bf16)


def local(sources, projection, translations, angles, interpolation, box_order):
    box_count, sides, points = sources.shape
    coeffs = projection.shape[1] // 2
    count_x, count_y = lax.axis_size("gx"), lax.axis_size("gy")
    per_peer = box_count // count_y
    levels = translations.shape[0]
    chunks = per_peer * SPLITS
    rows = 2 * sides // SPLITS
    slots = jnp.arange(box_count, dtype=jnp.int32)
    inverse = jnp.sum(
        jnp.where((box_order % box_count)[None, :] == slots[:, None], slots[None, :], 0), axis=1
    ).astype(jnp.int32)
    later = angles[1:].reshape(levels, count_y, per_peer, coeffs).transpose(1, 2, 0, 3)
    later = later.reshape(count_y, per_peer * levels, coeffs)
    weights = translations.reshape(levels, 2, 2, coeffs, 2 * coeffs)
    vmem = pl.BlockSpec(memory_space=pltpu.VMEM)
    state = pltpu.VMEM((chunks, count_y, rows, coeffs), jnp.bfloat16)
    single = pltpu.VMEM((count_y, rows, coeffs), jnp.bfloat16)
    phases = pltpu.VMEM((count_y, per_peer * levels, coeffs), jnp.float32)
    dma = pltpu.SemaphoreType.DMA
    return pl.pallas_call(
        functools.partial(kernel, count_x, count_y, per_peer, sides),
        out_shape=jax.ShapeDtypeStruct((box_count, 2 * sides, points), jnp.bfloat16),
        in_specs=[pl.BlockSpec(memory_space=pltpu.SMEM)] + [vmem] * 7,
        out_specs=vmem,
        scratch_shapes=[state] * 6 + [single] * 2 + [phases] * 3 + [
            dma((chunks, count_y)), dma((chunks, count_y)),
            dma((count_y,)), dma((count_y,)),
            dma((2, chunks)), dma((2, chunks)),
        ],
        compiler_params=pltpu.CompilerParams(
            collective_id=0, has_side_effects=True, vmem_limit_bytes=60 * 2**20
        ),
    )(
        inverse, sources, projection, weights, jnp.cos(angles[0]), jnp.sin(angles[0]),
        later, interpolation,
    )


def solution(mesh):
    placed = (
        P(("gx", "gy"), None, None),
        P(),
        P(),
        P(None, ("gx", "gy"), None),
        P(),
        P(("gx", "gy")),
    )
    return jax.shard_map(
        local, mesh=mesh, in_specs=placed, out_specs=P(("gx", "gy"), None, None), check_vma=False
    )
```

```python
import functools

import jax
import jax.numpy as jnp
from jax import lax
from jax.experimental import pallas as pl
from jax.experimental.pallas import tpu as pltpu
from jax.sharding import PartitionSpec as P

SPLITS = 2
LAG_X = 2
LAG_END = 4


def level_plan(count_x, count_y):
    bits_x = count_x.bit_length() - 1
    bits_y = count_y.bit_length() - 1
    return [
        ("gy", bits_y - 1),
        ("gx", bits_x - 1),
        ("gy", bits_y - 2),
        ("gx", bits_x - 2),
        ("gy", bits_y - 3),
    ]


def kernel(
    count_x, count_y, per_peer, sides,
    inv_ref, src_ref, proj_ref, w_ref, cos0_ref, sin0_ref, ang_ref,
    out_ref,
    st0, got0, st1, got1, st2, got2, tmp_a, wx, ang_got, cs, sn,
    a2a_send, a2a_recv, ang_send, ang_recv, ex_send, ex_recv,
):
    f32, bf16 = jnp.float32, jnp.bfloat16
    plan = level_plan(count_x, count_y)
    levels = len(plan)
    me_x = lax.axis_index("gx")
    me_y = lax.axis_index("gy")
    half = sides // SPLITS
    rows = 2 * half
    coeffs = st0.shape[-1]
    chunks = per_peer * SPLITS
    x_bits = [bit for axis, bit in plan if axis == "gx"]
    x_levels = [level for level, (axis, bit) in enumerate(plan) if axis == "gx"]
    x_hbs = [(me_x // (1 << bit)) % 2 for bit in x_bits]
    partners = [me_x + (1 - 2 * hb) * (1 << bit) for hb, bit in zip(x_hbs, x_bits)]

    barrier = pltpu.get_barrier_semaphore()
    for k in range(1, count_y):
        pl.semaphore_signal(
            barrier, inc=1, device_id=(me_x, (me_y + k) % count_y),
            device_id_type=pl.DeviceIdType.MESH,
        )
    for partner in partners:
        pl.semaphore_signal(
            barrier, inc=1, device_id=(partner, me_y), device_id_type=pl.DeviceIdType.MESH
        )
    pl.semaphore_wait(barrier, count_y - 1 + len(partners))

    def ang_copy(k):
        peer = (me_y + k) % count_y
        return pltpu.make_async_remote_copy(
            src_ref=ang_ref.at[peer], dst_ref=ang_got.at[me_y],
            send_sem=ang_send.at[k], recv_sem=ang_recv.at[k],
            device_id=(me_x, peer), device_id_type=pl.DeviceIdType.MESH,
        )

    def a2a_copy(c, k):
        peer = (me_y + k) % count_y
        return pltpu.make_async_remote_copy(
            src_ref=st0.at[c, peer], dst_ref=got0.at[c, me_y],
            send_sem=a2a_send.at[c, k], recv_sem=a2a_recv.at[c, k],
            device_id=(me_x, peer), device_id_type=pl.DeviceIdType.MESH,
        )

    def swap_copy(which, c):
        source, target = ((st1, got1), (st2, got2))[which]
        return pltpu.make_async_remote_copy(
            src_ref=source.at[c], dst_ref=target.at[c],
            send_sem=ex_send.at[which, c], recv_sem=ex_recv.at[which, c],
            device_id=(partners[which], me_y), device_id_type=pl.DeviceIdType.MESH,
        )

    for k in range(1, count_y):
        ang_copy(k).start()
    ang_got[me_y] = ang_ref[me_y]

    for which, (level, hb) in enumerate(zip(x_levels, x_hbs)):
        own = pl.multiple_of(hb * coeffs, coeffs)
        rest = pl.multiple_of((1 - hb) * coeffs, coeffs)
        wx[which, :coeffs, :] = w_ref[level, hb, pl.ds(own, coeffs), :]
        wx[which, coeffs:, :] = w_ref[level, hb, pl.ds(rest, coeffs), :]

    def put(store, real, imag, cosine, sine):
        store(0, (cosine * real - sine * imag).astype(bf16))
        store(half, (sine * real + cosine * imag).astype(bf16))

    def project(c):
        r, q = c // SPLITS, c % SPLITS
        first = pl.multiple_of(q * half, half)
        group = jnp.concatenate(
            [src_ref[inv_ref[p * per_peer + r], pl.ds(first, half), :] for p in range(count_y)],
            axis=0,
        )
        prod = jnp.dot(group, proj_ref[...], preferred_element_type=f32)
        for p in range(count_y):
            block = prod[p * half : (p + 1) * half]

            def store(at, value, p=p):
                st0[c, p, at : at + half, :] = value

            slot = p * per_peer + r
            put(
                store, block[:, :coeffs], block[:, coeffs:],
                cos0_ref[pl.ds(slot, 1), :], sin0_ref[pl.ds(slot, 1), :],
            )

    def finish(prod, index, y, r, level, store):
        base = index * rows
        upper = prod[base : base + half]
        lower = prod[base + half : base + rows]
        real = upper[:, :coeffs] - lower[:, coeffs:]
        imag = lower[:, :coeffs] + upper[:, coeffs:]
        row = r * levels + level
        put(store, real, imag, cs[y, pl.ds(row, 1), :], sn[y, pl.ds(row, 1), :])

    def y_level(load, make_store, level, r):
        stride = 1 << plan[level][1]
        lows = [y for y in range(count_y) if (y // stride) % 2 == 0]
        low = jnp.concatenate([load(y) for y in lows], axis=0)
        high = jnp.concatenate([load(y + stride) for y in lows], axis=0)
        joined = jnp.concatenate([low, high], axis=1)
        for h in range(2):
            prod = jnp.dot(joined, w_ref[level, h], preferred_element_type=f32)
            for index, y in enumerate(lows):
                finish(prod, index, y + h * stride, r, level, make_store(y + h * stride))

    def x_level(mine, other, which, r, make_store):
        joined = jnp.concatenate([mine, other], axis=1)
        prod = jnp.dot(joined, wx[which], preferred_element_type=f32)
        for y in range(count_y):
            finish(prod, y, y, r, x_levels[which], make_store(y))

    def into(ref):
        def make_store(y):
            def store(at, value):
                ref[y, at : at + half, :] = value

            return store

        return make_store

    def into_chunk(ref, c):
        def make_store(y):
            def store(at, value):
                ref[c, y, at : at + half, :] = value

            return store

        return make_store

    def flat(value):
        return value.reshape(count_y * rows, coeffs)

    @pl.loop(0, chunks)
    def _(c):
        project(c)
        for k in range(1, count_y):
            a2a_copy(c, k).start()
        got0[c, me_y] = st0[c, me_y]

    for k in range(1, count_y):
        ang_copy(k).wait()
    for y in range(count_y):
        angle = ang_got[y]
        cs[y] = jnp.cos(angle)
        sn[y] = jnp.sin(angle)

    @pl.loop(0, chunks + LAG_END)
    def _(t):
        @pl.when(t < chunks)
        def _():
            c = t
            for k in range(1, count_y):
                a2a_copy(c, k).wait()
            y_level(lambda y: got0[c, y], into_chunk(st1, c), 0, c // SPLITS)
            swap_copy(0, c).start()

        @pl.when((t >= LAG_X) & (t < chunks + LAG_X))
        def _():
            c = t - LAG_X
            r = c // SPLITS
            swap_copy(0, c).wait()
            x_level(flat(st1[c]), flat(got1[c]), 0, r, into(tmp_a))
            y_level(lambda y: tmp_a[y], into_chunk(st2, c), 2, r)
            swap_copy(1, c).start()

        @pl.when(t >= LAG_END)
        def _():
            c = t - LAG_END
            r, q = c // SPLITS, c % SPLITS
            swap_copy(1, c).wait()
            x_level(flat(st2[c]), flat(got2[c]), 1, r, into(tmp_a))
            first = pl.multiple_of(q * half, half)

            def make_store(y):
                def store(at, value):
                    begin = first if at == 0 else first + sides
                    out_ref[y * per_peer + r, pl.ds(begin, half), :] = value

                return store

            y_level(lambda y: tmp_a[y], make_store, 4, r)


def interpolate_kernel(state_ref, interp_ref, out_ref):
    group, rows, coeffs = state_ref.shape
    sides, points = rows // 2, interp_ref.shape[1] // 2
    prod = jnp.dot(
        state_ref[...].reshape(group * rows, coeffs), interp_ref[...],
        preferred_element_type=jnp.float32,
    )
    for g in range(group):
        upper = prod[g * rows : g * rows + sides]
        lower = prod[g * rows + sides : (g + 1) * rows]
        real = upper[:, :points] - lower[:, points:]
        imag = upper[:, points:] + lower[:, :points]
        out_ref[g, :sides, :] = real.astype(out_ref.dtype)
        out_ref[g, sides:, :] = imag.astype(out_ref.dtype)


def local(sources, projection, translations, angles, interpolation, box_order):
    box_count, sides, points = sources.shape
    coeffs = projection.shape[1] // 2
    count_x, count_y = lax.axis_size("gx"), lax.axis_size("gy")
    per_peer = box_count // count_y
    levels = translations.shape[0]
    chunks = per_peer * SPLITS
    rows = 2 * sides // SPLITS
    slots = jnp.arange(box_count, dtype=jnp.int32)
    inverse = jnp.sum(
        jnp.where((box_order % box_count)[None, :] == slots[:, None], slots[None, :], 0), axis=1
    ).astype(jnp.int32)
    later = angles[1:].reshape(levels, count_y, per_peer, coeffs).transpose(1, 2, 0, 3)
    later = later.reshape(count_y, per_peer * levels, coeffs)
    vmem = pl.BlockSpec(memory_space=pltpu.VMEM)
    state = pltpu.VMEM((chunks, count_y, rows, coeffs), jnp.bfloat16)
    single = pltpu.VMEM((count_y, rows, coeffs), jnp.bfloat16)
    phases = pltpu.VMEM((count_y, per_peer * levels, coeffs), jnp.float32)
    dma = pltpu.SemaphoreType.DMA
    state_out = pl.pallas_call(
        functools.partial(kernel, count_x, count_y, per_peer, sides),
        out_shape=jax.ShapeDtypeStruct((box_count, 2 * sides, coeffs), jnp.bfloat16),
        in_specs=[pl.BlockSpec(memory_space=pltpu.SMEM)] + [vmem] * 6,
        out_specs=vmem,
        scratch_shapes=[state] * 6 + [single] + [pltpu.VMEM((2, 2 * coeffs, 2 * coeffs), jnp.bfloat16)] + [phases] * 3 + [
            dma((chunks, count_y)), dma((chunks, count_y)),
            dma((count_y,)), dma((count_y,)),
            dma((2, chunks)), dma((2, chunks)),
        ],
        compiler_params=pltpu.CompilerParams(
            collective_id=0, has_side_effects=True, vmem_limit_bytes=60 * 2**20
        ),
    )(
        inverse, sources, projection, translations, jnp.cos(angles[0]), jnp.sin(angles[0]),
        later,
    )
    group = 4
    return pl.pallas_call(
        interpolate_kernel,
        out_shape=jax.ShapeDtypeStruct((box_count, 2 * sides, points), jnp.bfloat16),
        grid=(box_count // group,),
        in_specs=[
            pl.BlockSpec((group, 2 * sides, coeffs), lambda i: (i, 0, 0)),
            pl.BlockSpec(interpolation.shape, lambda i: (0, 0)),
        ],
        out_specs=pl.BlockSpec((group, 2 * sides, points), lambda i: (i, 0, 0)),
    )(state_out, interpolation)


def solution(mesh):
    placed = (
        P(("gx", "gy"), None, None),
        P(),
        P(),
        P(None, ("gx", "gy"), None),
        P(),
        P(("gx", "gy")),
    )
    return jax.shard_map(
        local, mesh=mesh, in_specs=placed, out_specs=P(("gx", "gy"), None, None), check_vma=False
    )
```
